32 devices in a mesh: dp: 8 (over z, y), mp: 4 (over x, core).
Axes of the slice: x: 2, y: 2, z: 4, core: 2. Of those that a mesh axis runs over, the one named last changes fastest.
Arguments:
- hidden: bfloat16 [16384, 768], P(('dp', 'mp')), may hold values from -6 to 6
- char_ids: int32 [16384, 16], P(('dp', 'mp')), may hold values from 0 to 999
- segments: int32 [32, 512], P('dp'), may hold values from 0 to 7, never falling along the last dimension, each value on 1 to 128 neighbouring positions
- attn_in: bfloat16 [768, 3, 768], P('dp', None, 'mp'), may hold values from -0.21875 to 0.21875
- attn_bias: bfloat16 [2, 768], replicated, may hold values from -3 to 3
- attn_out: bfloat16 [768, 768], P('mp', 'dp'), may hold values from -0.875 to 0.875
- proj_bias: bfloat16 [4, 768], replicated, may hold values from -3 to 3
- norm_gain: bfloat16 [4, 768], replicated, may hold values from 0.5 to 1.5
- norm_shift: bfloat16 [4, 768], replicated, may hold values from -3 to 3
- stream_maps: bfloat16 [1536, 768], P('dp', 'mp'), may hold values from -0.21875 to 0.21875
- merging_kernel: bfloat16 [4608, 1536], P('dp', 'mp'), may hold values from -0.09375 to 0.09375
- merging_bias: bfloat16 [1536], replicated, may hold values from -3 to 3
- ffn_up: bfloat16 [768, 3072], P('dp', 'mp'), may hold values from -0.21875 to 0.21875
- ffn_bias: bfloat16 [3072], replicated, may hold values from -3 to 3
- ffn_down: bfloat16 [3072, 768], P('mp', 'dp'), may hold values from -0.109375 to 0.109375
- gru_input: bfloat16 [2, 256, 1152], replicated, may hold values from -0.375 to 0.375
- gru_state: bfloat16 [2, 384, 1152], replicated, may hold values from -0.3125 to 0.3125
- gru_bias: bfloat16 [2, 2, 1152], replicated, may hold values from -3 to 3
- char_table: bfloat16 [1000, 256], replicated, may hold values from -6 to 6
- tok_grad: bfloat16 [16384, 768], P(('dp', 'mp')), may hold values from -6 to 6
- char_grad: bfloat16 [16384, 768], P(('dp', 'mp')), may hold values from -6 to 6
Outputs:
- tok_out: bfloat16 [16384, 768], P(('dp', 'mp'))
- char_out: bfloat16 [16384, 768], P(('dp', 'mp'))
- hidden_grad: float32 [16384, 768], P(('dp', 'mp'))
- grad_attn_in: float32 [768, 3, 768], P('dp', None, 'mp')
- grad_attn_bias: float32 [2, 768], replicated
- grad_attn_out: float32 [768, 768], P('mp', 'dp')
- grad_proj_bias: float32 [4, 768], replicated
- grad_gain: float32 [4, 768], replicated
- grad_shift: float32 [4, 768], replicated
- grad_maps: float32 [1536, 768], P('dp', 'mp')
- grad_kernel: float32 [4608, 1536], P('dp', 'mp')
- grad_merging_bias: float32 [1536], replicated
- grad_ffn_up: float32 [768, 3072], P('dp', 'mp')
- grad_ffn_bias: float32 [3072], replicated
- grad_ffn_down: float32 [3072, 768], P('mp', 'dp')
- grad_gru_input: float32 [2, 256, 1152], replicated
- grad_gru_state: float32 [2, 384, 1152], replicated
- grad_gru_bias: float32 [2, 2, 1152], replicated
- grad_table: float32 [1000, 256], replicated
The draws below stay inside these ranges and needn't reach their ends.
Inputs may be any that keep to these rules, and one draw needn't show every extreme that they name: `segments`: in each sequence the numbers never fall; one run of a number has 1 to 128 positions.
All inputs are finite; a program needn't handle non-finite values.
Results may differ from the reference program's by a relative error of at most 0.02.
Values may be sent and summed in bfloat16 or wider, within the bound.
A program may use at most 512 MiB of HBM per device.

```python
import math
import jax
import jax.numpy as jnp
import numpy as np
from jax import lax

D = 768
HEADS = 12
HEAD = 64
FF = 3072
H = 384
CE = 256
VC = 1000
CHARS = 16
LEN = 512
SEQS = 32
TOKENS = 16384


def plant(drawn, stream_key, smallest, top_value):
    extent = drawn.shape
    index_at = [jax.random.randint(jax.random.fold_in(stream_key, axis), (), 0, extent[axis]) for axis in range(len(extent))]
    drawn = drawn.at[tuple(index_at)].set(smallest)
    longest = extent.index(max(extent))
    index_at[longest] = (index_at[longest] + 1) % extent[longest]
    return drawn.at[tuple(index_at)].set(top_value)


def steps_of(stream_key, shape, split, low, high):
    level = 1.0
    for axis_at, blocks in split:
        draws = jax.random.uniform(jax.random.fold_in(jax.random.fold_in(stream_key, 6), axis_at), (blocks,), jnp.float32, low / len(split), high / len(split))
        level = level * jnp.repeat(jnp.exp(draws), shape[axis_at] // blocks).reshape((-1,) + (1,) * (len(shape) - 1 - axis_at))
    return level


def length_profile(count, total, most, skew):
    weights = [(1 << 20) // math.isqrt(standing ** skew) + 1 for standing in range(2, count + 1)]
    rest, given = total - most - (count - 1), [1] * (count - 1)
    while rest > 0:
        candidates = [i for i in range(count - 1) if given[i] < most]
        mass, left = sum([weights[i] for i in candidates]), rest
        for i in candidates:
            more = min(most - given[i], max(1, left * weights[i] // mass), rest)
            given[i] = given[i] + more
            rest = rest - more
    return np.array([most] + given)


def uneven_parts(own_key, count, total, limit, lean):
    if count == 2:
        one = jax.random.randint(own_key, (), max(1, total - limit), min(limit, total - 1) + 1)
        return jnp.stack([one, total - one])
    lengths = jnp.asarray(length_profile(count, total, limit, lean), jnp.int32)
    twos = (count - 1) // 2
    source_of, receiver = lengths[1:1 + 2 * twos:2], lengths[2:2 + 2 * twos:2]
    margin = jnp.minimum(source_of - 1, limit - receiver)
    moved = jax.random.randint(jax.random.fold_in(own_key, 1), (twos,), 0, 1 << 20) % (margin + 1)
    lengths = lengths.at[1:1 + 2 * twos:2].set(source_of - moved).at[2:2 + 2 * twos:2].set(receiver + moved)
    return lengths[jax.random.permutation(jax.random.fold_in(own_key, 2), count)]


def centred(own_key, extent, spread, reach, cuts=(), kind=jnp.bfloat16):
    entries = jax.random.normal(own_key, extent, jnp.float32) * spread
    if len(cuts) > 0:
        entries = steps_of(own_key, extent, cuts, -0.22, 0.18) * entries
    return jnp.clip(entries, min=-reach, max=reach).astype(kind)


def setup_inputs(seed: int = 0) -> dict:
    arg_keys = jax.random.split(jax.random.key(seed), 22)
    hidden = centred(arg_keys[0], (TOKENS, D), 1.0, 6.0, ((0, 32),))
    char_ids = plant(jax.random.randint(arg_keys[1], (TOKENS, CHARS), 0, VC), jax.random.fold_in(arg_keys[1], 1), 0, VC - 1).astype(jnp.int32)
    segments = jax.vmap(lambda own: jnp.searchsorted(jnp.cumsum(uneven_parts(own, 8, LEN, LEN // 4, 0)), jnp.arange(LEN), side="right"))(jax.random.split(arg_keys[2], SEQS)).reshape((SEQS, LEN)).astype(jnp.int32)
    attn_in = centred(arg_keys[3], (D, 3, D), D ** -0.5, 0.21875, ((0, 8), (2, 4)))
    attn_bias = centred(arg_keys[4], (2, D), 0.5, 3.0)
    attn_out = centred(arg_keys[5], (D, D), (D // 16) ** -0.5, 0.875, ((0, 4), (1, 8)))
    proj_bias = centred(arg_keys[6], (4, D), 0.5, 3.0)
    norm_gain = jnp.clip(1.0 + 0.1 * jax.random.normal(arg_keys[7], (4, D), jnp.float32), 0.5, 1.5).astype(jnp.bfloat16)
    norm_shift = centred(arg_keys[8], (4, D), 0.5, 3.0)
    stream_maps = centred(arg_keys[9], (2 * D, D), D ** -0.5, 0.21875, ((0, 8), (1, 4)))
    merging_kernel = centred(arg_keys[10], (6 * D, 2 * D), (6 * D) ** -0.5, 0.09375, ((0, 8), (1, 4)))
    merging_bias = centred(arg_keys[11], (2 * D,), 0.5, 3.0)
    ffn_up = centred(arg_keys[12], (D, FF), D ** -0.5, 0.21875, ((0, 8), (1, 4)))
    ffn_bias = centred(arg_keys[13], (FF,), 0.5, 3.0)
    ffn_down = centred(arg_keys[14], (FF, D), FF ** -0.5, 0.109375, ((0, 4), (1, 8)))
    gru_input = centred(arg_keys[15], (2, CE, 3 * H), CE ** -0.5, 0.375)
    gru_state = centred(arg_keys[16], (2, H, 3 * H), H ** -0.5, 0.3125)
    gru_bias = centred(arg_keys[17], (2, 2, 3 * H), 0.5, 3.0)
    char_table = centred(arg_keys[18], (VC, CE), 1.0, 6.0)
    tok_grad = centred(arg_keys[19], (TOKENS, D), 1.0, 6.0, ((0, 32),))
    char_grad = centred(arg_keys[20], (TOKENS, D), 1.0, 6.0, ((0, 32),))
    return {"hidden": hidden, "char_ids": char_ids, "segments": segments, "attn_in": attn_in, "attn_bias": attn_bias, "attn_out": attn_out, "proj_bias": proj_bias, "norm_gain": norm_gain, "norm_shift": norm_shift, "stream_maps": stream_maps, "merging_kernel": merging_kernel, "merging_bias": merging_bias, "ffn_up": ffn_up, "ffn_bias": ffn_bias, "ffn_down": ffn_down, "gru_input": gru_input, "gru_state": gru_state, "gru_bias": gru_bias, "char_table": char_table, "tok_grad": tok_grad, "char_grad": char_grad}


@jax.custom_vjp
def low(v):
    return lax.optimization_barrier(v.astype(jnp.bfloat16)).astype(jnp.float32)

@jax.custom_vjp
def low_back(v):
    return v

def low_keep(v):
    return (low(v), None)

def low_pass(kept, grad):
    return (grad,)

def back_keep(v):
    return (v, None)

def back_low(kept, grad):
    return (low(grad),)
low.defvjp(low_keep, low_pass)
low_back.defvjp(back_keep, back_low)
EPSILON = 1e-12
MASKED = -1e+30
HIGH = lax.Precision.HIGHEST

def matmul(left, right):
    return jnp.dot(left, right, precision=HIGH)

def norm_rows(values, gain, shift):
    center = values - lax.optimization_barrier(jnp.mean(values, axis=-1, keepdims=True))
    invert = lax.rsqrt(lax.optimization_barrier(jnp.mean(center * center, axis=-1, keepdims=True)) + EPSILON)
    return center * invert * gain + shift

def neighbours(joined, segs):
    same = segs[:, 1:] == segs[:, :-1]
    edge = segs[:, :1] != segs[:, :1]
    has_prev = jnp.concatenate([edge, same], axis=1)
    has_next = jnp.concatenate([same, edge], axis=1)
    zero_row = jnp.zeros_like(joined[:, :1])
    before = jnp.concatenate([zero_row, joined[:, :-1]], axis=1)
    after = jnp.concatenate([joined[:, 1:], zero_row], axis=1)
    before = jnp.where(has_prev[..., None], before, jnp.zeros_like(before))
    after = jnp.where(has_next[..., None], after, jnp.zeros_like(after))
    return jnp.concatenate([before, joined, after], axis=-1)

def forward_block(params, hidden, chars, segs):
    attn_in, attn_bias, attn_out, proj_bias, norm_gain, norm_shift, stream_maps, merging_kernel, merging_bias, ffn_up, ffn_bias, ffn_down, gru_input, gru_state, gru_bias, char_table = params
    nseq = segs.shape[0]
    nrows = nseq * LEN
    queries = low(low_back(matmul(hidden, attn_in[:, 0]) + attn_bias[0]))
    keys_in = low(low_back(matmul(hidden, attn_in[:, 1])))
    values_in = low(low_back(matmul(hidden, attn_in[:, 2]) + attn_bias[1]))

    def split_heads(values):
        return values.reshape(nseq, LEN, HEADS, HEAD)
    scores = jnp.einsum('sqhe,skhe->shqk', split_heads(queries), split_heads(keys_in), precision=HIGH)
    scores = low_back(scores * HEAD ** (-0.5))
    same = segs[:, :, None] == segs[:, None, :]
    scores = jnp.where(same[:, None], scores, MASKED)
    probs = low(jax.nn.softmax(scores, axis=-1))
    context = jnp.einsum('shqk,skhe->sqhe', probs, split_heads(values_in), precision=HIGH).reshape(nrows, D)
    context = low(low_back(context))
    attn = low_back(matmul(context, attn_out) + proj_bias[0])
    after_attn = norm_rows(hidden + attn, norm_gain[0], norm_shift[0])
    embedded = char_table[chars]
    ordered = jnp.moveaxis(jnp.stack([embedded, embedded[:, ::-1]], axis=0), 2, 0)

    def gru_step(state, inputs):
        proj_in = low_back(jnp.einsum('drc,dcg->drg', inputs, gru_input, precision=HIGH) + gru_bias[:, 0][:, None, :])
        proj_rec = low_back(jnp.einsum('drh,dhg->drg', low(state), gru_state, precision=HIGH) + gru_bias[:, 1][:, None, :])
        reset = jax.nn.sigmoid(proj_in[..., :H] + proj_rec[..., :H])
        update = jax.nn.sigmoid(proj_in[..., H:2 * H] + proj_rec[..., H:2 * H])
        fresh = jnp.tanh(proj_in[..., 2 * H:] + reset * proj_rec[..., 2 * H:])
        return ((1.0 - update) * fresh + update * state, None)
    final, unused = lax.scan(gru_step, jnp.zeros((2, nrows, H), jnp.float32), ordered)
    char_hidden = jnp.concatenate([final[0], final[1]], axis=-1)
    token_map = matmul(low(after_attn), stream_maps[:D]) + proj_bias[1]
    char_map = matmul(low(char_hidden), stream_maps[D:]) + proj_bias[2]
    joined = low(low_back(jnp.concatenate([token_map, char_map], axis=-1)))
    stacked = neighbours(joined.reshape(nseq, LEN, 2 * D), segs).reshape(nrows, 6 * D)
    merged_pre = low_back(matmul(stacked, merging_kernel) + merging_bias)
    merged = jax.nn.gelu(merged_pre, approximate=False)
    mixed = norm_rows(after_attn + merged[:, :D], norm_gain[1], norm_shift[1])
    char_out = norm_rows(char_hidden + merged[:, D:], norm_gain[3], norm_shift[3])
    inner_pre = low_back(matmul(low(mixed), ffn_up) + ffn_bias)
    inner = low(jax.nn.gelu(inner_pre, approximate=False))
    ffn_val = low_back(matmul(inner, ffn_down) + proj_bias[3])
    tok_out = norm_rows(mixed + ffn_val, norm_gain[2], norm_shift[2])
    return (tok_out, char_out)

def reference(hidden, char_ids, segments, attn_in, attn_bias, attn_out, proj_bias, norm_gain, norm_shift, stream_maps, merging_kernel, merging_bias, ffn_up, ffn_bias, ffn_down, gru_input, gru_state, gru_bias, char_table, tok_grad, char_grad):
    params = tuple((p.astype(jnp.float32) for p in (attn_in, attn_bias, attn_out, proj_bias, norm_gain, norm_shift, stream_maps, merging_kernel, merging_bias, ffn_up, ffn_bias, ffn_down, gru_input, gru_state, gru_bias, char_table)))
    per_block = math.gcd(SEQS, 4)
    blocks = SEQS // per_block
    block_rows = per_block * LEN

    def one_block(carry, index):
        start = (index * block_rows).astype(jnp.int32)
        seq_start = (index * per_block).astype(jnp.int32)
        tokens = lax.dynamic_slice_in_dim(hidden, start, block_rows, 0).astype(jnp.float32)
        chars = lax.dynamic_slice_in_dim(char_ids, start, block_rows, 0)
        segs = lax.dynamic_slice_in_dim(segments, seq_start, per_block, 0)
        cot_tok = lax.dynamic_slice_in_dim(tok_grad, start, block_rows, 0).astype(jnp.float32)
        cot_char = lax.dynamic_slice_in_dim(char_grad, start, block_rows, 0).astype(jnp.float32)

        def run(weights, tokens_in):
            return forward_block(weights, tokens_in, chars, segs)
        outputs, pull = jax.vjp(run, params, tokens)
        weight_grads, token_grads = pull((cot_tok, cot_char))
        carry = jax.tree.map(jnp.add, carry, weight_grads)
        return (carry, (outputs[0].astype(jnp.bfloat16), outputs[1].astype(jnp.bfloat16), token_grads))
    zeros = tuple((jnp.zeros_like(p) for p in params))
    grads, stacked_out = lax.scan(one_block, zeros, jnp.arange(blocks, dtype=jnp.int32))
    tok_out = stacked_out[0].reshape(TOKENS, D)
    char_out = stacked_out[1].reshape(TOKENS, D)
    hidden_grad = stacked_out[2].reshape(TOKENS, D)
    return (tok_out, char_out, hidden_grad, grads[0], grads[1], grads[2], grads[3], grads[4], grads[5], grads[6], grads[7], grads[8], grads[9], grads[10], grads[11], grads[12], grads[13], grads[14], grads[15])
```

```python
import functools

import jax
import jax.numpy as jnp
from jax import lax
from jax.experimental import pallas as pl
from jax.experimental.pallas import tpu as pltpu
from jax.sharding import PartitionSpec as P

HEAD = 64
H = 384
LEN = 512
PACK = 384

EPSILON = 1e-12
MASKED = -1e30
LOW = jnp.bfloat16
WIDE = jnp.float32


def widen(values):
    return values.astype(jnp.float32)


def dot(left, right):
    return jnp.dot(left, right, preferred_element_type=jnp.float32)


def dot_nt(left, right):
    return lax.dot_general(
        left, right, (((1,), (1,)), ((), ())), preferred_element_type=jnp.float32
    )


def dot_tn(left, right):
    return lax.dot_general(
        left, right, (((0,), (0,)), ((), ())), preferred_element_type=jnp.float32
    )


def gru_fwd_body(
    emb0, emb1, w_in, w_rec, bias, out_prev, out_reset, out_update, out_fresh, out_rec, out_last,
    state
):
    @pl.when(pl.program_id(0) == 0)
    def _():
        state[...] = jnp.zeros_like(state)

    for d, emb in enumerate((emb0, emb1)):
        prev = state[d]
        prev_low = prev.astype(LOW)
        proj_in = dot(emb[0], w_in[d]) + bias[d, 0:1]
        proj_rec = dot(prev_low, w_rec[d]) + bias[d, 1:2]
        gates = 0.5 + 0.5 * jnp.tanh(0.5 * (proj_in[:, : 2 * H] + proj_rec[:, : 2 * H]))
        reset = gates[:, :H]
        update = gates[:, H:]
        rec_fresh = proj_rec[:, 2 * H :]
        fresh = jnp.tanh(proj_in[:, 2 * H :] + reset * rec_fresh)
        state[d] = fresh + update * (prev - fresh)
        out_prev[0, d] = prev_low
        out_reset[0, d] = reset.astype(LOW)
        out_update[0, d] = update.astype(LOW)
        out_fresh[0, d] = fresh.astype(LOW)
        out_rec[0, d] = rec_fresh.astype(LOW)
    out_last[...] = state[...]


def whole(shape):
    zeros = (0,) * len(shape)
    return pl.BlockSpec(shape, lambda *_: zeros)


def gru_forward(emb, w_in, w_rec, bias):
    steps, rows, width = emb.shape
    kept = jax.ShapeDtypeStruct((steps, 2, rows, H), LOW)
    kept_spec = pl.BlockSpec((1, 2, rows, H), lambda t: (t, 0, 0, 0))
    return pl.pallas_call(
        gru_fwd_body,
        grid=(steps,),
        in_specs=[
            pl.BlockSpec((1, rows, width), lambda t: (t, 0, 0)),
            pl.BlockSpec((1, rows, width), lambda t: (steps - 1 - t, 0, 0)),
            whole(w_in.shape),
            whole(w_rec.shape),
            whole(bias.shape),
        ],
        out_specs=[kept_spec] * 5 + [whole((2, rows, H))],
        out_shape=[kept] * 5 + [jax.ShapeDtypeStruct((2, rows, H), WIDE)],
        scratch_shapes=[pltpu.VMEM((2, rows, H), WIDE)],
        compiler_params=pltpu.CompilerParams(vmem_limit_bytes=56 << 20),
        cost_estimate=pl.CostEstimate(
            flops=steps * 4 * rows * 3 * H * (width + H),
            transcendentals=steps * 6 * rows * H,
            bytes_accessed=steps * rows * H * 20,
        ),
        name="gru_forward",
    )(emb, emb, w_in, w_rec, bias)


def gru_bwd_body(
    last, start, start_in, start_rec, start_bias, emb0, emb1, prev_ref, reset_ref, update_ref,
    fresh_ref, rec_ref, w_in_t, w_rec_t, grad_emb0, grad_emb1, *outs_and_scratch
):
    if last:
        out_grad, acc_bias, acc_in, acc_rec, grad_state = outs_and_scratch
    else:
        grad_state, acc_in, acc_rec, acc_bias = outs_and_scratch

    @pl.when(pl.program_id(0) == 0)
    def _():
        grad_state[...] = start[...]
        acc_in[...] = start_in[...]
        acc_rec[...] = start_rec[...]
        acc_bias[...] = start_bias[...]

    for d, (emb, grad_emb) in enumerate(((emb0, grad_emb0), (emb1, grad_emb1))):
        grad = grad_state[d]
        prev_low = prev_ref[0, d]
        prev = widen(prev_low)
        reset = widen(reset_ref[0, d])
        update = widen(update_ref[0, d])
        fresh = widen(fresh_ref[0, d])
        rec_fresh = widen(rec_ref[0, d])
        kept = grad * update
        pre_fresh = (grad - kept) * (1.0 - fresh * fresh)
        hidden_part = pre_fresh * reset
        pre_reset = hidden_part * rec_fresh * (1.0 - reset)
        pre_update = kept * (prev - fresh) * (1.0 - update)
        low_reset = pre_reset.astype(LOW)
        low_update = pre_update.astype(LOW)
        low_fresh = pre_fresh.astype(LOW)
        low_part = hidden_part.astype(LOW)
        grad_in = jnp.concatenate([low_reset, low_update, low_fresh], axis=-1)
        grad_rec = jnp.concatenate([low_reset, low_update, low_part], axis=-1)
        grad_state[d] = kept + dot(grad_rec, w_rec_t[d])
        grad_emb[0] = dot(grad_in, w_in_t[d]).astype(LOW)
        acc_rec[d] += dot_tn(prev_low, grad_rec)
        acc_in[d] += dot_tn(emb[0], grad_in)
        sum_reset = jnp.sum(widen(low_reset), axis=0, keepdims=True)
        sum_update = jnp.sum(widen(low_update), axis=0, keepdims=True)
        sum_fresh = jnp.sum(widen(low_fresh), axis=0, keepdims=True)
        sum_part = jnp.sum(widen(low_part), axis=0, keepdims=True)
        acc_bias[d, 0:1] += jnp.concatenate([sum_reset, sum_update, sum_fresh], axis=-1)
        acc_bias[d, 1:2] += jnp.concatenate([sum_reset, sum_update, sum_part], axis=-1)

    if last:

        @pl.when(pl.program_id(0) == pl.num_programs(0) - 1)
        def _():
            width = acc_in.shape[1]
            out_grad[:, :width] = acc_in[...].astype(LOW)
            out_grad[:, width:] = acc_rec[...].astype(LOW)


def gru_backward(part, parts, carry, emb, saved, w_in_t, w_rec_t):
    steps, rows, width = emb.shape
    count = steps // parts
    top = steps - 1 - part * count
    gates = 3 * H
    last = part == parts - 1
    kept_spec = pl.BlockSpec((1, 2, rows, H), lambda t: (top - t, 0, 0, 0))
    back = pl.BlockSpec((1, rows, width), lambda t: (top - t, 0, 0))
    fore = pl.BlockSpec((1, rows, width), lambda t: (steps - 1 - top + t, 0, 0))
    back_out = pl.BlockSpec((1, rows, width), lambda t: (count - 1 - t, 0, 0))
    fore_out = pl.BlockSpec((1, rows, width), lambda t: (t, 0, 0))
    accs = [(2, rows, H), (2, width, gates), (2, H, gates), (2, 2, gates)]
    if last:
        shapes = [
            jax.ShapeDtypeStruct((2, width + H, gates), LOW),
            jax.ShapeDtypeStruct(accs[3], WIDE),
        ]
        scratch = [pltpu.VMEM(accs[1], WIDE), pltpu.VMEM(accs[2], WIDE), pltpu.VMEM(accs[0], WIDE)]
    else:
        shapes = [jax.ShapeDtypeStruct(acc, WIDE) for acc in accs]
        scratch = []
    return pl.pallas_call(
        functools.partial(gru_bwd_body, last),
        grid=(count,),
        in_specs=[whole(acc) for acc in accs]
        + [back, fore]
        + [kept_spec] * 5
        + [whole(w_in_t.shape), whole(w_rec_t.shape)],
        out_specs=[back_out, fore_out] + [whole(shape.shape) for shape in shapes],
        out_shape=[jax.ShapeDtypeStruct((count, rows, width), LOW)] * 2 + shapes,
        scratch_shapes=scratch,
        compiler_params=pltpu.CompilerParams(vmem_limit_bytes=60 << 20),
        cost_estimate=pl.CostEstimate(
            flops=count * 8 * rows * gates * (width + H),
            transcendentals=0,
            bytes_accessed=count * rows * H * 20,
        ),
        name="gru_backward",
    )(*carry, emb, emb, *saved, w_in_t, w_rec_t)


BAND = 128


def band(block, length):
    return max(0, (block - 1) * BAND), min(length, (block + 2) * BAND)


def half_mask(part, width):
    lanes = lax.broadcasted_iota(jnp.int32, (1, width), 1)
    return (lanes >= part * HEAD) & (lanes < (part + 1) * HEAD)


def take_half(values, part):
    return jnp.where(half_mask(part, values.shape[1]), values, jnp.zeros_like(values))


def block_probs(queries, keys, seg_rows, seg_cols):
    scores = dot_nt(queries, keys) * HEAD ** (-0.5)
    scores = jnp.where(seg_rows == seg_cols, scores, MASKED)
    expo = jnp.exp(scores - jnp.max(scores, axis=-1, keepdims=True))
    return expo / jnp.sum(expo, axis=-1, keepdims=True)


def attend_body(q_ref, k_ref, v_ref, seg_rows, seg_cols, out_ref):
    length = q_ref.shape[0]
    for block in range(length // BAND):
        rows = pl.ds(block * BAND, BAND)
        low, high = band(block, length)
        keys = k_ref[low:high]
        values = v_ref[low:high]
        total = jnp.zeros((BAND, q_ref.shape[1]), WIDE)
        for part in range(2):
            probs = block_probs(
                take_half(q_ref[rows], part), keys, seg_rows[rows], seg_cols[:, low:high]
            )
            total += dot(probs.astype(LOW), take_half(values, part))
        out_ref[rows] = total.astype(LOW)


def attend_back_body(
    q_ref, k_ref, v_ref, g_ref, seg_rows, seg_cols, gq_ref, gk_ref, gv_ref, acc_k, acc_v
):
    length, width = q_ref.shape
    acc_k[...] = jnp.zeros_like(acc_k)
    acc_v[...] = jnp.zeros_like(acc_v)
    scale = HEAD ** (-0.5)
    for block in range(length // BAND):
        rows = pl.ds(block * BAND, BAND)
        low, high = band(block, length)
        keys = k_ref[low:high]
        values = v_ref[low:high]
        total = jnp.zeros((BAND, width), WIDE)
        for part in range(2):
            queries = take_half(q_ref[rows], part)
            upstream = take_half(g_ref[rows], part)
            probs = block_probs(queries, keys, seg_rows[rows], seg_cols[:, low:high])
            grad_probs = dot_nt(upstream, values)
            inner = probs * grad_probs
            grad_scores = (inner - probs * jnp.sum(inner, axis=-1, keepdims=True)).astype(LOW)
            acc_v[low:high] += dot_tn(probs.astype(LOW), upstream)
            acc_k[low:high] += dot_tn(grad_scores, queries)
            total += dot(grad_scores, take_half(keys, part))
        gq_ref[rows] = (total * scale).astype(LOW)
    gk_ref[...] = (acc_k[...] * scale).astype(LOW)
    gv_ref[...] = acc_v[...].astype(LOW)


def attend_specs(length, count):
    pair = pl.BlockSpec((length, 2 * HEAD), lambda s, h: (s, h))
    return [pair] * count + [
        pl.BlockSpec((length, 1), lambda s, h: (s, 0)),
        pl.BlockSpec((None, 1, length), lambda s, h: (s, 0, 0)),
    ]


def attend(queries, keys, values, segs):
    rows, width = queries.shape
    count = segs.shape[0]
    return pl.pallas_call(
        attend_body,
        grid=(count, width // (2 * HEAD)),
        in_specs=attend_specs(LEN, 3),
        out_specs=pl.BlockSpec((LEN, 2 * HEAD), lambda s, h: (s, h)),
        out_shape=jax.ShapeDtypeStruct((rows, width), LOW),
        cost_estimate=pl.CostEstimate(
            flops=4 * rows * LEN * width, transcendentals=rows * LEN * width // HEAD,
            bytes_accessed=rows * width * 8,
        ),
        name="attend",
    )(queries, keys, values, segs.reshape(-1, 1), segs[:, None, :])


def attend_back(queries, keys, values, upstream, segs):
    rows, width = queries.shape
    count = segs.shape[0]
    pair = pl.BlockSpec((LEN, 2 * HEAD), lambda s, h: (s, h))
    return pl.pallas_call(
        attend_back_body,
        grid=(count, width // (2 * HEAD)),
        in_specs=attend_specs(LEN, 4),
        out_specs=[pair] * 3,
        out_shape=[jax.ShapeDtypeStruct((rows, width), LOW)] * 3,
        scratch_shapes=[pltpu.VMEM((LEN, 2 * HEAD), WIDE)] * 2,
        cost_estimate=pl.CostEstimate(
            flops=10 * rows * LEN * width, transcendentals=rows * LEN * width // HEAD,
            bytes_accessed=rows * width * 14,
        ),
        name="attend_back",
    )(queries, keys, values, upstream, segs.reshape(-1, 1), segs[:, None, :])


def norm_stats(values):
    center = values - jnp.mean(values, axis=-1, keepdims=True)
    invert = lax.rsqrt(jnp.mean(center * center, axis=-1, keepdims=True) + EPSILON)
    return center * invert, invert


def norm_rows(values, gain, shift):
    normed, _ = norm_stats(values)
    return normed * gain + shift


def norm_back(values, upstream, gain):
    normed, invert = norm_stats(values)
    scaled = upstream * gain
    inner = (
        scaled
        - jnp.mean(scaled, axis=-1, keepdims=True)
        - normed * jnp.mean(scaled * normed, axis=-1, keepdims=True)
    )
    return (inner * invert, jnp.sum(upstream * normed, axis=0), jnp.sum(upstream, axis=0))


def gelu_both(values):
    cumul = 0.5 * (1.0 + lax.erf(values * 0.7071067811865476))
    slope = cumul + values * jnp.exp(-0.5 * values * values) * 0.3989422804014327
    return values * cumul, slope


def edge_masks(segs):
    same = segs[:, 1:] == segs[:, :-1]
    edge = segs[:, :1] != segs[:, :1]
    return (jnp.concatenate([edge, same], axis=1), jnp.concatenate([same, edge], axis=1))


def neighbours(joined, segs):
    has_prev, has_next = edge_masks(segs)
    zero_row = jnp.zeros_like(joined[:, :1])
    before = jnp.concatenate([zero_row, joined[:, :-1]], axis=1)
    after = jnp.concatenate([joined[:, 1:], zero_row], axis=1)
    before = jnp.where(has_prev[..., None], before, jnp.zeros_like(before))
    after = jnp.where(has_next[..., None], after, jnp.zeros_like(after))
    return jnp.concatenate([before, joined, after], axis=-1)


def fold(block):
    rows, cols = block.shape
    if cols < PACK:
        share = PACK // cols
        return jnp.concatenate(
            [block[i * (rows // share) : (i + 1) * (rows // share)] for i in range(share)], axis=1
        )
    return jnp.concatenate([block[:, i : i + PACK] for i in range(0, cols, PACK)], axis=0)


def unfold(packed, cols):
    if cols < PACK:
        return jnp.concatenate(
            [packed[..., i : i + cols] for i in range(0, PACK, cols)], axis=-2
        )
    share = cols // PACK
    rows = packed.shape[-2] // share
    return jnp.concatenate(
        [packed[..., i * rows : (i + 1) * rows, :] for i in range(share)], axis=-1
    )


def gather_packed(blocks):
    packed = jnp.concatenate([fold(block) for block in blocks], axis=0)
    return lax.all_gather(packed, ("mp", "dp"), axis=0)


def rows_of(block):
    return block.shape[0] * block.shape[1] // PACK


def copy_body(shapes, packed, *outs):
    at = 0
    for (rows, cols), out in zip(shapes, outs):
        size = rows * cols // PACK
        for j in range(packed.shape[0]):
            block = packed[j, 0, at : at + size]
            if cols < PACK:
                share = PACK // cols
                for i in range(share):
                    out[i * size : (i + 1) * size, j * cols : (j + 1) * cols] = block[
                        :, i * cols : (i + 1) * cols
                    ]
            else:
                for i in range(cols // PACK):
                    left = j * cols + i * PACK
                    out[:, left : left + PACK] = block[i * rows : (i + 1) * rows]
        at += size


def unpack_all(gathered, blocks, dp, mp):
    total = gathered.shape[1]
    gathered = gathered.reshape(mp, dp, total, PACK)
    shapes = [block.shape for block in blocks]
    if all(rows_of(block) % 16 == 0 and block.shape[0] % 16 == 0 for block in blocks):
        return pl.pallas_call(
            functools.partial(copy_body, shapes),
            grid=(dp,),
            in_specs=[pl.BlockSpec((mp, 1, total, PACK), lambda i: (0, i, 0, 0))],
            out_specs=[pl.BlockSpec((r, mp * c), lambda i: (i, 0)) for r, c in shapes],
            out_shape=[jax.ShapeDtypeStruct((dp * r, mp * c), LOW) for r, c in shapes],
            compiler_params=pltpu.CompilerParams(vmem_limit_bytes=48 << 20),
            cost_estimate=pl.CostEstimate(
                flops=0, transcendentals=0, bytes_accessed=4 * gathered.size
            ),
            name="unpack",
        )(gathered)
    at = 0
    out = []
    for block in blocks:
        rows, cols = block.shape
        part = unfold(gathered[:, :, at : at + rows_of(block)], cols)
        at += rows_of(block)
        out.append(part.transpose(1, 2, 0, 3).reshape(dp * rows, mp * cols))
    return out


def swap(values, axis, size, mask):
    return lax.ppermute(values, axis, [(i, i ^ mask) for i in range(size)])


def pick(values, index, axis):
    return lax.dynamic_index_in_dim(values, index, axis, keepdims=False)


def bit_groups(size):
    groups = []
    low = 0
    take = 1
    while (1 << low) < size:
        bits = min(take, size.bit_length() - 1 - low)
        groups.append((low, bits))
        low += bits
        take = 2
    return groups


def start_halve(values, at, axis, size, low, bits):
    count = 1 << bits
    shape = values.shape
    view = values.reshape(shape[:at] + (shape[at] // count, count) + shape[at + 1 :])
    me = (lax.axis_index(axis) >> low) & (count - 1)
    mine = pick(view, me, at + 1)
    parts = [
        swap(pick(view, me ^ other, at + 1), axis, size, other << low)
        for other in range(1, count)
    ]
    return mine, parts


def total_of(mine, parts):
    total = widen(mine)
    for part in parts:
        total = total + widen(part)
    return total


def start_spread(values, axis, size, low, bits):
    return [swap(values, axis, size, other << low) for other in range(1, 1 << bits)]


def end_spread(values, parts, axis, low, bits):
    count = 1 << bits
    me = (lax.axis_index(axis) >> low) & (count - 1)
    parts = jnp.stack([values] + parts, axis=0)
    return jnp.stack([pick(parts, me ^ i, 0) for i in range(count)], axis=0)


class Flight:
    def __init__(self, steps):
        self.steps = steps
        self.result = None
        self.pending = next(steps)

    def land(self, values):
        try:
            self.pending = self.steps.send(values)
        except StopIteration as stop:
            self.pending = None
            self.result = stop.value


def land(anchor, *flights):
    flights = [flight for flight in flights if flight.pending is not None]
    anchor, pending = lax.optimization_barrier((anchor, [flight.pending for flight in flights]))
    for flight, values in zip(flights, pending):
        flight.land(values)
    return anchor


def finish(flight):
    while flight.pending is not None:
        flight.land(flight.pending)
    return flight.result


def sum_weight(block_of, rows, dp, mp, orders):
    rank = lax.axis_index("mp")
    away = [swap(block_of(rank ^ mask).astype(LOW), "mp", mp, 1) for mask in (1, 3)]
    away = yield away
    home = [
        (block_of(rank ^ mask) + widen(part)).astype(LOW) for mask, part in zip((0, 2), away)
    ]
    home = [part.reshape(dp, rows // dp, part.shape[-1]) for part in home]
    (low, bits), *rest = bit_groups(dp)
    share = dp // len(orders)
    cuts = [[part[i * share : (i + 1) * share] for part in home] for i in range(len(orders))]

    def over_y(part):
        return start_halve(part, 0, "dp", dp, low, bits)

    kept = []
    flying = []
    for x_first, (near, far) in zip(orders, cuts):
        if x_first:
            kept.append(near)
            flying.append([swap(far, "mp", mp, 2)])
        else:
            mine_near, parts_near = over_y(near)
            mine_far, parts_far = over_y(far)
            kept.append([mine_near, mine_far])
            flying.append([parts_near, parts_far])
    landed = yield flying
    flying = []
    for i, x_first in enumerate(orders):
        if x_first:
            total = total_of(kept[i], landed[i]).astype(LOW)
            kept[i], parts = over_y(total)
            flying.append(parts)
        else:
            near, far = [
                total_of(mine, parts).astype(LOW) for mine, parts in zip(kept[i], landed[i])
            ]
            kept[i] = near
            flying.append([swap(far, "mp", mp, 2)])
    landed = yield flying
    total = jnp.concatenate([total_of(k, parts) for k, parts in zip(kept, landed)], axis=0)
    for low, bits in rest:
        mine, parts = start_halve(total.astype(LOW), 0, "dp", dp, low, bits)
        parts = yield parts
        total = total_of(mine, parts)
    return total[0]


def sum_whole(values, dp, mp):
    rows, cols = values.shape[1:]
    mine, parts = start_halve(values, 0, "mp", mp, 0, 1)
    parts = yield parts
    total = total_of(mine, parts)[0].astype(LOW)
    groups = [("mp", mp, 1, 1)] + [("dp", dp) + group for group in bit_groups(dp)]
    done = []
    for axis, size, low, bits in groups:
        count = 1 << bits
        if total.shape[0] % (count * 8) == 0:
            mine, parts = start_halve(total.reshape(count, -1, cols), 0, axis, size, low, bits)
            parts = yield parts
            total = total_of(mine, parts)[0].astype(LOW)
            done.append((axis, size, low, bits))
        else:
            for bit in range(low, low + bits):
                parts = yield [swap(total, axis, size, 1 << bit)]
                total = total_of(total, parts).astype(LOW)
    for axis, size, low, bits in reversed(done):
        parts = yield start_spread(total, axis, size, low, bits)
        total = end_spread(total, parts, axis, low, bits).reshape(-1, cols)
    parts = yield start_spread(total, "mp", mp, 0, 1)
    return end_spread(total, parts, "mp", 0, 1)


def sum_small(parts, dp, mp):
    flat = jnp.concatenate([part.reshape(-1, 128) for part in parts], axis=0)
    for axis, size in (("mp", mp), ("dp", dp)):
        mask = 1
        while mask < size:
            got = yield [swap(flat, axis, size, mask)]
            flat = flat + got[0]
            mask *= 2
    out = []
    at = 0
    for part in parts:
        rows = part.size // 128
        out.append(flat[at : at + rows].reshape(part.shape))
        at += rows
    return out


def per_device(
    dp,
    mp,
    hidden,
    char_ids,
    segments,
    attn_in,
    attn_bias,
    attn_out,
    proj_bias,
    norm_gain,
    norm_shift,
    stream_maps,
    merging_kernel,
    merging_bias,
    ffn_up,
    ffn_bias,
    ffn_down,
    gru_input,
    gru_state,
    gru_bias,
    char_table,
    tok_grad,
    char_grad,
):
    mp_rank = lax.axis_index("mp")
    tok_rows, width = hidden.shape
    seq_count = tok_rows // LEN
    vocab_size = char_table.shape[0]
    chars = char_ids.shape[1]
    segs = lax.dynamic_slice_in_dim(segments, mp_rank * seq_count, seq_count, 0)
    gains = widen(norm_gain)
    shifts = widen(norm_shift)
    biases = widen(proj_bias)
    bias_attn = widen(attn_bias)

    in_rows, _, in_cols = attn_in.shape
    first_blocks = [attn_in[:, i] for i in range(3)] + [attn_out.T]
    later_blocks = [merging_kernel, ffn_up, ffn_down.T, stream_maps]
    first_all = gather_packed(first_blocks)
    later_all = gather_packed(later_blocks)

    ids_flat = char_ids.T.reshape(-1)
    vocab_pad = -(-vocab_size // 128) * 128
    table_pad = jnp.pad(char_table, ((0, vocab_pad - vocab_size), (0, 0)))
    one_hot = (ids_flat[:, None] == jnp.arange(vocab_pad, dtype=jnp.int32)[None, :]).astype(LOW)
    emb = dot(one_hot, table_pad).astype(LOW).reshape(chars, tok_rows, -1)
    *saved, final = gru_forward(emb, gru_input, gru_state, widen(gru_bias))
    char_hidden = jnp.concatenate([final[0], final[1]], axis=-1)
    char_low = char_hidden.astype(LOW)

    w_query, w_key, w_value, w_out_t = unpack_all(first_all, first_blocks, dp, mp)
    queries = (dot(hidden, w_query) + bias_attn[0]).astype(LOW)
    keys = dot(hidden, w_key).astype(LOW)
    values = (dot(hidden, w_value) + bias_attn[1]).astype(LOW)
    context = attend(queries, keys, values, segs)
    attn_pre = widen(hidden) + (dot_nt(context, w_out_t) + biases[0])
    after_attn = norm_rows(attn_pre, gains[0], shifts[0])
    after_low = after_attn.astype(LOW)

    kernel, w_up, w_down_t, maps = unpack_all(later_all, later_blocks, dp, mp)
    token_map = dot(after_low, maps[:width]) + biases[1]
    char_map = dot(char_low, maps[width:]) + biases[2]
    joined = jnp.concatenate([token_map, char_map], axis=-1).astype(LOW)
    stacked = neighbours(joined.reshape(seq_count, LEN, 2 * width), segs).reshape(
        tok_rows, 6 * width
    )
    merged_pre = dot(stacked, kernel) + widen(merging_bias)
    merged, merged_slope = gelu_both(merged_pre)
    mixed_pre = after_attn + merged[:, :width]
    mixed = norm_rows(mixed_pre, gains[1], shifts[1])
    char_pre = char_hidden + merged[:, width:]
    char_out = norm_rows(char_pre, gains[3], shifts[3]).astype(LOW)

    mixed_low = mixed.astype(LOW)
    inner_pre = dot(mixed_low, w_up) + widen(ffn_bias)
    inner, inner_slope = gelu_both(inner_pre)
    inner = inner.astype(LOW)
    ffn_val = dot_nt(inner, w_down_t) + biases[3]
    out_pre = mixed + ffn_val
    tok_out = norm_rows(out_pre, gains[2], shifts[2]).astype(LOW)
    grad_out2, gain_two, shift_two = norm_back(out_pre, widen(tok_grad), gains[2])
    grad_ffn_val = grad_out2.astype(LOW)
    bias_three = jnp.sum(widen(grad_ffn_val), axis=0)
    grad_inner_pre = (dot(grad_ffn_val, w_down_t) * inner_slope).astype(LOW)
    unit_bias_grad = jnp.sum(widen(grad_inner_pre), axis=0)

    def columns(values, index, size):
        return lax.dynamic_slice_in_dim(values, index * size, size, 1)

    unit_cols = ffn_up.shape[1]
    down_flight = Flight(
        sum_weight(
            lambda j: dot_tn(grad_ffn_val, columns(inner, j, unit_cols)), width, dp, mp, (True,)
        )
    )
    up_flight = Flight(
        sum_weight(
            lambda j: dot_tn(mixed_low, columns(grad_inner_pre, j, unit_cols)),
            width,
            dp,
            mp,
            (False,),
        )
    )
    grad_mixed = grad_out2 + dot_nt(grad_inner_pre, w_up)

    grad_mixed_pre, gain_one, shift_one = norm_back(mixed_pre, grad_mixed, gains[1])
    grad_char_pre, gain_four, shift_four = norm_back(char_pre, widen(char_grad), gains[3])
    grad_merged = jnp.concatenate([grad_mixed_pre, grad_char_pre], axis=-1)
    grad_merged_pre = (grad_merged * merged_slope).astype(LOW)
    merging_bias_grad = jnp.sum(widen(grad_merged_pre), axis=0)
    out_cols = merging_kernel.shape[1]
    kernel_flight = Flight(
        sum_weight(
            lambda j: dot_tn(stacked, columns(grad_merged_pre, j, out_cols)),
            6 * width,
            dp,
            mp,
            (True, False),
        )
    )
    grad_stacked = dot_nt(grad_merged_pre, kernel)
    grad_stacked = land(grad_stacked, down_flight, up_flight)
    grad_stacked = grad_stacked.reshape(seq_count, LEN, 6 * width)
    has_prev, has_next = edge_masks(segs)
    from_prev = jnp.where(has_prev[..., None], grad_stacked[..., : 2 * width], 0.0)
    from_next = jnp.where(has_next[..., None], grad_stacked[..., 4 * width :], 0.0)
    zero_row = jnp.zeros_like(from_prev[:, :1])
    grad_joined = (
        grad_stacked[..., 2 * width : 4 * width]
        + jnp.concatenate([from_prev[:, 1:], zero_row], axis=1)
        + jnp.concatenate([zero_row, from_next[:, :-1]], axis=1)
    )
    grad_joined = grad_joined.reshape(tok_rows, 2 * width).astype(LOW)
    joined_sums = jnp.sum(widen(grad_joined), axis=0)
    bias_one = joined_sums[:width]
    bias_two = joined_sums[width:]
    grad_after = grad_mixed_pre + dot_nt(grad_joined[:, :width], maps[:width])
    grad_char = grad_char_pre + dot_nt(grad_joined[:, width:], maps[width:])
    map_cols = stream_maps.shape[1]
    joined_token = grad_joined[:, :width]
    joined_char = grad_joined[:, width:]
    maps_flight = Flight(
        sum_weight(
            lambda j: jnp.concatenate(
                [
                    dot_tn(after_low, columns(joined_token, j, map_cols)),
                    dot_tn(char_low, columns(joined_char, j, map_cols)),
                ],
                axis=0,
            ),
            2 * width,
            dp,
            mp,
            (True,),
        )
    )

    grad_attn_pre, gain_zero, shift_zero = norm_back(attn_pre, grad_after, gains[0])
    grad_attn = grad_attn_pre.astype(LOW)
    bias_zero = jnp.sum(widen(grad_attn), axis=0)

    start_grad = jnp.stack([grad_char[:, :H], grad_char[:, H:]], axis=0)
    start_grad = land(start_grad, kernel_flight)
    emb_width = gru_input.shape[1]
    w_in_t = jnp.swapaxes(gru_input, 1, 2)
    w_rec_t = jnp.swapaxes(gru_state, 1, 2)
    carry = [
        start_grad,
        jnp.zeros(gru_input.shape, WIDE),
        jnp.zeros(gru_state.shape, WIDE),
        jnp.zeros(gru_bias.shape, WIDE),
    ]
    late0, early1, *carry = gru_backward(0, 2, carry, emb, saved, w_in_t, w_rec_t)
    carry[0] = land(carry[0], down_flight, up_flight, kernel_flight, maps_flight)
    early0, late1, gru_local, gru_bias_local = gru_backward(
        1, 2, carry, emb, saved, w_in_t, w_rec_t
    )
    grad_emb = jnp.concatenate(
        [widen(early0) + widen(early1), widen(late0) + widen(late1)], axis=0
    )
    grad_emb = grad_emb.astype(LOW).reshape(chars * tok_rows, -1)
    gru_flight = Flight(sum_whole(gru_local, dp, mp))
    small_flight = Flight(
        sum_small(
            [
                jnp.stack([bias_zero, bias_one, bias_two, bias_three], axis=0),
                jnp.stack([gain_zero, gain_one, gain_two, gain_four], axis=0),
                jnp.stack([shift_zero, shift_one, shift_two, shift_four], axis=0),
                merging_bias_grad,
                unit_bias_grad,
                gru_bias_local,
            ],
            dp,
            mp,
        )
    )
    grad_emb = land(grad_emb, down_flight, up_flight, kernel_flight, maps_flight)
    table_local = dot_tn(one_hot, grad_emb).astype(LOW)
    table_local = land(table_local, gru_flight, small_flight)
    table_flight = Flight(sum_whole(table_local.reshape(2, vocab_pad // 2, -1), dp, mp))

    grad_attn, table_local = lax.optimization_barrier((grad_attn, table_local))
    out_flight = Flight(
        sum_weight(
            lambda j: dot_tn(grad_attn, columns(context, j, in_cols)), width, dp, mp, (False,)
        )
    )
    grad_context = dot(grad_attn, w_out_t).astype(LOW)
    grad_context = land(grad_context, out_flight, table_flight, small_flight)
    grad_queries, grad_keys, grad_values = attend_back(queries, keys, values, grad_context, segs)
    grad_queries = land(
        grad_queries, out_flight, table_flight, gru_flight, small_flight, down_flight, up_flight,
        maps_flight, kernel_flight
    )
    hidden_grad = (
        grad_attn_pre
        + dot_nt(grad_queries, w_query)
        + dot_nt(grad_keys, w_key)
        + dot_nt(grad_values, w_value)
    )
    ins_flight = Flight(
        sum_weight(
            lambda j: dot_tn(
                hidden,
                jnp.concatenate(
                    [columns(g, j, in_cols) for g in (grad_queries, grad_keys, grad_values)],
                    axis=1,
                ),
            ),
            width,
            dp,
            mp,
            (True,),
        )
    )
    qv_local = jnp.stack(
        [jnp.sum(widen(grad_queries), axis=0), jnp.sum(widen(grad_values), axis=0)], axis=0
    )

    qv_flight = Flight(sum_small([qv_local], dp, mp))
    down_t, up, kernel_g, maps_g, out_t, ins, gru_sum, table_g = [
        finish(flight)
        for flight in (
            down_flight, up_flight, kernel_flight, maps_flight, out_flight, ins_flight,
            gru_flight, table_flight
        )
    ]
    table_g = widen(table_g.reshape(vocab_pad, -1)[:vocab_size])
    gru_sum = widen(gru_sum)
    input_g = gru_sum[:, :emb_width]
    state_g = gru_sum[:, emb_width:]

    proj, gain, shift, merging, unit, bias_g = finish(small_flight)
    (qv,) = finish(qv_flight)
    return (
        tok_out,
        char_out,
        hidden_grad,
        ins.reshape(attn_in.shape),
        qv,
        out_t.T,
        proj,
        gain,
        shift,
        maps_g,
        kernel_g,
        merging,
        up,
        unit,
        down_t.T,
        input_g,
        state_g,
        bias_g,
        table_g,
    )


def solution(mesh):
    in_specs = (
        P(("dp", "mp"), None),
        P(("dp", "mp"), None),
        P("dp", None),
        P("dp", None, "mp"),
        P(),
        P("mp", "dp"),
        P(),
        P(),
        P(),
        P("dp", "mp"),
        P("dp", "mp"),
        P(),
        P("dp", "mp"),
        P(),
        P("mp", "dp"),
        P(),
        P(),
        P(),
        P(),
        P(("dp", "mp"), None),
        P(("dp", "mp"), None),
    )
    out_specs = (
        P(("dp", "mp"), None),
        P(("dp", "mp"), None),
        P(("dp", "mp"), None),
        P("dp", None, "mp"),
        P(),
        P("mp", "dp"),
        P(),
        P(),
        P(),
        P("dp", "mp"),
        P("dp", "mp"),
        P(),
        P("dp", "mp"),
        P(),
        P("mp", "dp"),
        P(),
        P(),
        P(),
        P(),
    )
    return jax.shard_map(
        functools.partial(per_device, mesh.shape["dp"], mesh.shape["mp"]),
        mesh=mesh,
        in_specs=in_specs,
        out_specs=out_specs,
        check_vma=False,
    )
```
